32 devices in a mesh: dp: 2 (over x), tp: 4 (over z), cp: 4 (over y, core).
Axes of the slice: x: 2, y: 2, z: 4, core: 2. Of those that a mesh axis runs over, the one named last changes fastest.
Arguments:
- hidden: bfloat16 [2048, 2304], P(('dp', 'cp')), parts along dimension 0
- positions: int32 [2048], P(('dp', 'cp')), parts along dimension 0
- w_q: bfloat16 [2, 2304, 2048], P(None, None, 'tp')
- w_k: bfloat16 [2, 2304, 1024], P(None, None, 'tp')
- w_v: bfloat16 [2, 2304, 1024], P(None, None, 'tp')
- w_o: bfloat16 [2, 2048, 2304], P(None, 'tp')
- w_gate: bfloat16 [2, 2304, 9216], P(None, None, 'tp')
- w_up: bfloat16 [2, 2304, 9216], P(None, None, 'tp')
- w_down: bfloat16 [2, 9216, 2304], P(None, 'tp')
- norm_gain: float32 [2, 4, 2304], replicated
- qk_gain: float32 [2, 2, 256], replicated
Outputs:
- output 1: bfloat16 [2048, 2304], P(('dp', 'cp')), parts along dimension 0
- output 2: bfloat16 [2, 2048, 4, 256], P(None, ('dp', 'cp'), 'tp'), parts along dimension 1
- output 3: bfloat16 [2, 2048, 4, 256], P(None, ('dp', 'cp'), 'tp'), parts along dimension 1
There are 2 independent parts. The reference program is written for one: setup_inputs(seed, part) draws one part's arguments, and reference() takes and returns one part's arrays. A program takes and returns all parts, laid end to end along the dimension named above; an argument that names none is the same for every part.
All inputs are finite; a program needn't handle non-finite values.
Results may differ from the reference program's by a relative error of at most 0.0166709.
Values are sent between devices in bfloat16 or wider.
A program may use at most 1 GiB of HBM per device.

```python
import jax
import jax.numpy as jnp
from jax import lax

D = 2304
HEADS = 8
KV_HEADS = 4
HEAD = 256
FF = 9216
WINDOW = 1024
TOKENS = 1024

EPS = 1e-6
THETAS = (10000.0, 1000000.0)
LAYER_WINDOWS = (WINDOW, TOKENS)
Q_BLOCK = min(32, TOKENS)


def normal_weight(key_in, arr_shape, fan_in):
    scale_val = fan_in ** -0.5
    return (jax.random.normal(key_in, arr_shape, jnp.float32) * scale_val).astype(jnp.bfloat16)


def setup_inputs(seed: int = 0, part: int = 0) -> dict:
    part_key = jax.random.fold_in(jax.random.key(seed), part)
    key_hidden, key_start = jax.random.split(part_key, 2)
    shared = jax.random.split(jax.random.key(seed + 1), 9)
    hidden = jax.random.normal(key_hidden, (TOKENS, D), jnp.float32).astype(jnp.bfloat16)
    start_pos = jax.random.randint(key_start, (), 0, 1024)
    positions = (start_pos + jnp.arange(TOKENS)).astype(jnp.int32)
    return {
        'hidden': hidden,
        'positions': positions,
        'w_q': normal_weight(shared[0], (2, D, HEADS * HEAD), D),
        'w_k': normal_weight(shared[1], (2, D, KV_HEADS * HEAD), D),
        'w_v': normal_weight(shared[2], (2, D, KV_HEADS * HEAD), D),
        'w_o': normal_weight(shared[3], (2, HEADS * HEAD, D), HEADS * HEAD),
        'w_gate': normal_weight(shared[4], (2, D, FF), D),
        'w_up': normal_weight(shared[5], (2, D, FF), D),
        'w_down': normal_weight(shared[6], (2, FF, D), FF),
        'norm_gain': 0.4 * jax.random.normal(shared[7], (2, 4, D), jnp.float32),
        'qk_gain': 0.4 * jax.random.normal(shared[8], (2, 2, HEAD), jnp.float32),
    }


def rms_scale(values, gain):
    mean_sq = jnp.mean(values * values, axis=-1, keepdims=True)
    return values * lax.rsqrt(mean_sq + EPS) * (1.0 + gain)


def rotary(values, positions, theta):
    half_dim = HEAD // 2
    inv_freq = theta ** (-(jnp.arange(half_dim, dtype=jnp.float32) * 2.0) / HEAD)
    angles = positions.astype(jnp.float32)[..., None] * inv_freq
    cosine = jnp.cos(angles)[..., None, :]
    sine_val = jnp.sin(angles)[..., None, :]
    lower_half = values[..., :half_dim]
    upper_half = values[..., half_dim:]
    return jnp.concatenate([lower_half * cosine - upper_half * sine_val, upper_half * cosine + lower_half * sine_val], axis=-1)


def attention(queries, key_rows, val_rows, window):
    groups = HEADS // KV_HEADS
    score_scale = HEAD ** -0.5
    key_f = key_rows.astype(jnp.float32)
    val_f = val_rows.astype(jnp.float32)
    q_blocks = queries.reshape(TOKENS // Q_BLOCK, Q_BLOCK, KV_HEADS, groups, HEAD)
    key_index = jnp.arange(TOKENS)

    def one_block(block_args):
        q_block, block_id = block_args
        scores = jnp.einsum('qhgd,uhd->hgqu', q_block.astype(jnp.float32), key_f) * score_scale
        query_index = block_id * Q_BLOCK + jnp.arange(Q_BLOCK)
        distance = query_index[:, None] - key_index[None, :]
        allowed = (distance >= 0) & (distance < window)
        scores = jnp.where(allowed, scores, -jnp.inf)
        prob_all = jax.nn.softmax(scores, axis=-1)
        return jnp.einsum('hgqu,uhd->qhgd', prob_all, val_f)

    block_out = lax.map(one_block, (q_blocks, jnp.arange(TOKENS // Q_BLOCK)))
    return block_out.reshape(TOKENS, HEADS * HEAD).astype(jnp.bfloat16)


def reference(hidden, positions, w_q, w_k, w_v, w_o, w_gate, w_up, w_down, norm_gain, qk_gain):
    state_f = hidden.astype(jnp.float32)
    new_hidden = hidden
    k_list = []
    v_list = []
    for layer_id in range(2):
        layer_gain = norm_gain[layer_id]
        normed = rms_scale(state_f, layer_gain[0]).astype(jnp.bfloat16)
        q_proj = jnp.dot(normed, w_q[layer_id], preferred_element_type=jnp.float32).reshape(TOKENS, HEADS, HEAD)
        k_proj = jnp.dot(normed, w_k[layer_id], preferred_element_type=jnp.float32).reshape(TOKENS, KV_HEADS, HEAD)
        v_rows = jnp.dot(normed, w_v[layer_id], preferred_element_type=jnp.float32).astype(jnp.bfloat16).reshape(TOKENS, KV_HEADS, HEAD)
        q_rot = rotary(rms_scale(q_proj, qk_gain[layer_id, 0]), positions, THETAS[layer_id]).astype(jnp.bfloat16)
        k_rot = rotary(rms_scale(k_proj, qk_gain[layer_id, 1]), positions, THETAS[layer_id]).astype(jnp.bfloat16)
        attn_rows = attention(q_rot, k_rot, v_rows, LAYER_WINDOWS[layer_id])
        attn_out = jnp.dot(attn_rows, w_o[layer_id], preferred_element_type=jnp.float32)
        resid_f = (state_f + rms_scale(attn_out, layer_gain[1])).astype(jnp.bfloat16).astype(jnp.float32)
        normed_mlp = rms_scale(resid_f, layer_gain[2]).astype(jnp.bfloat16)
        gate_proj = jnp.dot(normed_mlp, w_gate[layer_id], preferred_element_type=jnp.float32)
        up_proj = jnp.dot(normed_mlp, w_up[layer_id], preferred_element_type=jnp.float32)
        act_rows = (jax.nn.gelu(gate_proj, approximate=True) * up_proj).astype(jnp.bfloat16)
        mlp_out = jnp.dot(act_rows, w_down[layer_id], preferred_element_type=jnp.float32)
        new_hidden = (resid_f + rms_scale(mlp_out, layer_gain[3])).astype(jnp.bfloat16)
        state_f = new_hidden.astype(jnp.float32)
        k_list.append(k_rot)
        v_list.append(v_rows)
    return new_hidden, jnp.stack(k_list), jnp.stack(v_list)
```

```python
import functools
import jax
import jax.numpy as jnp
from jax import lax
from jax.experimental import pallas as pl
from jax.experimental.pallas import tpu as pltpu
from jax.sharding import PartitionSpec as P

MESH = pl.DeviceIdType.MESH
THETAS = (10000.0, 1000000.0)
EPS = 1e-6
NEG_BIG = -1e30
TOK = 256
D = 2304
HEAD = 256
HALF = 128
Q_HEADS = 2
FT = 256
NFT = D // FT
RS = 8
NRS = 128 // RS
AG = 16
NAG = 128 // AG
F32 = jnp.float32
BF16 = jnp.bfloat16


def norm_rows(src, gain, dst, rows=16):
    def body(i, carry):
        sl = pl.ds(pl.multiple_of(i * rows, rows), rows)
        vals = src[sl, :].astype(F32)
        mean_sq = jnp.mean(vals * vals, axis=-1, keepdims=True)
        dst[sl, :] = (vals * lax.rsqrt(mean_sq + EPS) * gain).astype(BF16)
        return carry

    lax.fori_loop(0, TOK // rows, body, 0)


def head_norm_rope(vals, gain, cosine, sine):
    mean_sq = jnp.mean(vals * vals, axis=-1, keepdims=True)
    vals = vals * lax.rsqrt(mean_sq + EPS) * gain
    low, high = vals[:, :HALF], vals[:, HALF:]
    return jnp.concatenate([low * cosine - high * sine, high * cosine + low * sine], axis=-1).astype(BF16)


def reduce_norm_share(z, part, land, res, gain, out, sems):
    rs_send, rs_recv, ag_send, ag_recv = sems

    def towards(flow):
        return z + 1 if flow else z - 1

    def away(flow):
        return z - 1 if flow else z + 1

    def rs_copy(flow, c):
        rows = pl.ds(pl.multiple_of(128 * flow + c * RS, RS), RS)
        return pltpu.make_async_remote_copy(
            src_ref=part.at[rows], dst_ref=land.at[rows], send_sem=rs_send.at[flow, c],
            recv_sem=rs_recv.at[flow, c], device_id={'tp': towards(flow)}, device_id_type=MESH)

    def ag_copy(flow, c):
        rows = pl.ds(pl.multiple_of(128 * flow + c * AG, AG), AG)
        return pltpu.make_async_remote_copy(
            src_ref=out.at[rows], dst_ref=out.at[rows], send_sem=ag_send.at[flow, c],
            recv_sem=ag_recv.at[flow, c], device_id={'tp': away(flow)}, device_id_type=MESH)

    def take(flow, c):
        rs_copy(flow, c).wait_recv()
        rows = pl.ds(pl.multiple_of(128 * flow + c * RS, RS), RS)
        part[rows, :] = part[rows, :] + land[rows, :]

    def hop(flow, c):
        take(flow, c)
        rs_copy(flow, c).start()

    def relay(flow, c):
        ag_copy(flow, c).wait_recv()
        ag_copy(flow, c).start()

    def loop(n, fn, start=0):
        def body(i, carry):
            fn(i)
            return carry
        lax.fori_loop(start, n, body, 0)

    def end_role(source, final):
        loop(NRS, lambda c: rs_copy(source, c).start())

        def finish(c):
            for i in range(AG // RS):
                take(final, c * (AG // RS) + i)
            rows = pl.ds(pl.multiple_of(128 * final + c * AG, AG), AG)
            vals = part[rows, :]
            mean_sq = jnp.mean(vals * vals, axis=-1, keepdims=True)
            out[rows, :] = (res[rows, :].astype(F32) + vals * lax.rsqrt(mean_sq + EPS) * gain).astype(BF16)
            ag_copy(final, c).start()

        loop(NAG, finish)
        loop(NAG, lambda c: ag_copy(source, c).wait_recv())
        loop(NRS, lambda c: rs_copy(source, c).wait_send())
        loop(NAG, lambda c: ag_copy(final, c).wait_send())

    def mid_role(near, far):
        hop(near, 0)

        def both(c):
            hop(near, c)
            hop(far, c - 1)

        loop(NRS, both, 1)
        hop(far, NRS - 1)

        def both_ag(c):
            relay(far, c)
            relay(near, c)

        loop(NAG, both_ag)
        loop(NRS, lambda c: rs_copy(near, c).wait_send())
        loop(NRS, lambda c: rs_copy(far, c).wait_send())
        loop(NAG, lambda c: ag_copy(near, c).wait_send())
        loop(NAG, lambda c: ag_copy(far, c).wait_send())

    pl.when(z == 0)(lambda: end_role(1, 0))
    pl.when(z == 1)(lambda: mid_role(1, 0))
    pl.when(z == 2)(lambda: mid_role(0, 1))
    pl.when(z == 3)(lambda: end_role(0, 1))


def layer_kernel(layer, x_ref, rope_ref, wq_hbm, wk_hbm, wv_hbm, wo_hbm, wg_hbm, wu_hbm, wd_hbm, gain_ref, qk_ref,
                 x_out, k_out, v_out,
                 wq, wk, wv, wo, wg, wu, wd, h_buf, r_buf, s_buf, part, land, q_buf, kv, acc, run_max, run_sum,
                 w_sem, t_sem, kv_send, kv_recv, rs_send, rs_recv, ag_send, ag_recv):
    z = lax.axis_index('tp')
    me = lax.axis_index('cp')
    twin = me + 1 - 2 * lax.rem(me, 2)
    across = lax.rem(me + 2, 4)

    barrier = pltpu.get_barrier_semaphore()
    pl.when(z > 0)(lambda: pl.semaphore_signal(barrier, inc=1, device_id={'tp': z - 1}, device_id_type=MESH))
    pl.when(z < 3)(lambda: pl.semaphore_signal(barrier, inc=1, device_id={'tp': z + 1}, device_id_type=MESH))
    pl.semaphore_signal(barrier, inc=1, device_id={'cp': twin}, device_id_type=MESH)
    pl.semaphore_signal(barrier, inc=1, device_id={'cp': across}, device_id_type=MESH)

    loads = [pltpu.make_async_copy(src.at[layer], dst, w_sem.at[i])
             for i, (src, dst) in enumerate(((wk_hbm, wk), (wv_hbm, wv), (wq_hbm, wq), (wo_hbm, wo)))]
    for copy in loads:
        copy.start()

    def tile_load(kind, src, dst, t):
        cols = pl.ds(pl.multiple_of(t * FT, FT), FT)
        return pltpu.make_async_copy(src.at[layer, :, cols], dst.at[t], t_sem.at[kind, t])

    def start_gate_up(t, carry):
        tile_load(0, wg_hbm, wg, t).start()
        tile_load(1, wu_hbm, wu, t).start()
        return carry

    def start_down(t, carry):
        tile_load(2, wd_hbm, wd, t).start()
        return carry

    lax.fori_loop(0, NFT, start_gate_up, 0)
    lax.fori_loop(0, NFT, start_down, 0)

    gains = [1.0 + gain_ref[layer, i:i + 1, :] for i in range(4)]
    q_gain = 1.0 + qk_ref[layer, 0:1, :]
    k_gain = 1.0 + qk_ref[layer, 1:2, :]
    cosine, sine = rope_ref[layer, 0], rope_ref[layer, 1]

    norm_rows(x_ref, gains[0], h_buf)
    state = h_buf[...]

    loads[0].wait()
    k_rot = head_norm_rope(jnp.dot(state, wk[...], preferred_element_type=F32), k_gain, cosine, sine)
    kv[me, 0] = k_rot
    k_out[...] = k_rot
    loads[1].wait()
    v_rows = jnp.dot(state, wv[...], preferred_element_type=F32).astype(BF16)
    kv[me, 1] = v_rows
    v_out[...] = v_rows

    near_count = jnp.where(z > 0, 1, 0) + jnp.where(z < 3, 1, 0)
    pl.semaphore_wait(barrier, near_count + 2)

    def kv_copy(slot, part_id, lane, target):
        return pltpu.make_async_remote_copy(
            src_ref=kv.at[slot, part_id], dst_ref=kv.at[slot, part_id], send_sem=kv_send.at[lane, part_id],
            recv_sem=kv_recv.at[slot, part_id], device_id={'cp': target}, device_id_type=MESH)

    def send_own():
        for i in range(2):
            pl.when(me < 2)(lambda: kv_copy(me, i, 1, across).start())
            pl.when(lax.rem(me, 2) == 0)(lambda: kv_copy(me, i, 0, twin).start())

    send_own()

    loads[2].wait()
    q_all = jnp.dot(state, wq[...], preferred_element_type=F32)
    for i in range(Q_HEADS):
        q_buf[i * TOK:(i + 1) * TOK, :] = head_norm_rope(
            q_all[:, i * HEAD:(i + 1) * HEAD], q_gain, cosine, sine)

    def scores_of(slot):
        return lax.dot_general(q_buf[...], kv[slot, 0], (((1,), (1,)), ((), ())),
                               preferred_element_type=F32) * (HEAD ** -0.5)

    def first_block():
        scores = scores_of(me)
        row = lax.broadcasted_iota(jnp.int32, (Q_HEADS, TOK, TOK), 1).reshape(Q_HEADS * TOK, TOK)
        col = lax.broadcasted_iota(jnp.int32, (Q_HEADS * TOK, TOK), 1)
        scores = jnp.where(row >= col, scores, NEG_BIG)
        top = jnp.max(scores, axis=-1, keepdims=True)
        prob = jnp.exp(scores - top)
        run_max[...] = jnp.broadcast_to(top, run_max.shape)
        run_sum[...] = jnp.broadcast_to(jnp.sum(prob, axis=-1, keepdims=True), run_sum.shape)
        acc[...] = jnp.dot(prob.astype(BF16), kv[me, 1], preferred_element_type=F32)

    def next_block(slot):
        scores = scores_of(slot)
        old = run_max[:, :1]
        top = jnp.maximum(old, jnp.max(scores, axis=-1, keepdims=True))
        prob = jnp.exp(scores - top)
        factor = jnp.exp(old - top)
        run_max[...] = jnp.broadcast_to(top, run_max.shape)
        run_sum[...] = run_sum[...] * factor + jnp.sum(prob, axis=-1, keepdims=True)
        acc[...] = acc[...] * factor + jnp.dot(prob.astype(BF16), kv[slot, 1], preferred_element_type=F32)

    first_block()

    def recv(slot):
        for i in range(2):
            kv_copy(slot, i, 0, twin).wait_recv()

    def relay(slot):
        for i in range(2):
            kv_copy(slot, i, 0, twin).wait_recv()
            kv_copy(slot, i, 2, twin).start()

    def sent(lane, slot):
        for i in range(2):
            kv_copy(slot, i, lane, twin).wait_send()

    @pl.when(me == 0)
    def _():
        sent(0, 0)
        sent(1, 0)

    @pl.when(me == 1)
    def _():
        recv(0)
        next_block(0)
        sent(1, 1)

    @pl.when(me == 2)
    def _():
        relay(0)
        next_block(0)
        recv(1)
        next_block(1)
        sent(0, 2)
        sent(2, 0)

    @pl.when(me == 3)
    def _():
        recv(2)
        next_block(2)
        relay(1)
        next_block(1)
        recv(0)
        next_block(0)
        sent(2, 1)

    loads[3].wait()
    for i in range(Q_HEADS):
        rows = slice(i * TOK, (i + 1) * TOK)
        s_buf[:, i * HEAD:(i + 1) * HEAD] = (acc[rows, :] / run_sum[rows, :1]).astype(BF16)
    part[...] = jnp.dot(s_buf[:, :Q_HEADS * HEAD], wo[...], preferred_element_type=F32)

    def phase(n):
        return (rs_send.at[n], rs_recv.at[n], ag_send.at[n], ag_recv.at[n])

    reduce_norm_share(z, part, land, x_ref, gains[1], r_buf, phase(0))

    norm_rows(r_buf, gains[2], h_buf)

    def gate_up(t, carry):
        tile_load(0, wg_hbm, wg, t).wait()
        tile_load(1, wu_hbm, wu, t).wait()
        gate = jnp.dot(h_buf[...], wg[t], preferred_element_type=F32)
        up = jnp.dot(h_buf[...], wu[t], preferred_element_type=F32)
        s_buf[:, pl.ds(pl.multiple_of(t * FT, FT), FT)] = (jax.nn.gelu(gate, approximate=True) * up).astype(BF16)
        return carry

    lax.fori_loop(0, NFT, gate_up, 0)

    def down(t, carry):
        tile_load(2, wd_hbm, wd, t).wait()
        part[:, pl.ds(pl.multiple_of(t * FT, FT), FT)] = jnp.dot(s_buf[...], wd[t], preferred_element_type=F32)
        return carry

    lax.fori_loop(0, NFT, down, 0)

    reduce_norm_share(z, part, land, r_buf, gains[3], x_out, phase(1))


def run_layer(layer, x, rope, weights, norm_gain, qk_gain):
    vmem = pl.BlockSpec(memory_space=pltpu.VMEM)
    hbm = pl.BlockSpec(memory_space=pl.ANY)
    sem = pltpu.SemaphoreType.DMA
    return pl.pallas_call(
        functools.partial(layer_kernel, layer),
        name=f'layer_{layer}',
        out_shape=(
            jax.ShapeDtypeStruct((TOK, D), BF16),
            jax.ShapeDtypeStruct((TOK, HEAD), BF16),
            jax.ShapeDtypeStruct((TOK, HEAD), BF16),
        ),
        in_specs=[vmem, vmem] + [hbm] * 7 + [vmem, vmem],
        out_specs=(vmem, vmem, vmem),
        scratch_shapes=[
            pltpu.VMEM((D, Q_HEADS * HEAD), BF16),
            pltpu.VMEM((D, HEAD), BF16),
            pltpu.VMEM((D, HEAD), BF16),
            pltpu.VMEM((Q_HEADS * HEAD, D), BF16),
            pltpu.VMEM((NFT, D, FT), BF16),
            pltpu.VMEM((NFT, D, FT), BF16),
            pltpu.VMEM((NFT, D, FT), BF16),
            pltpu.VMEM((TOK, D), BF16),
            pltpu.VMEM((TOK, D), BF16),
            pltpu.VMEM((TOK, D), BF16),
            pltpu.VMEM((TOK, D), F32),
            pltpu.VMEM((TOK, D), F32),
            pltpu.VMEM((Q_HEADS * TOK, HEAD), BF16),
            pltpu.VMEM((4, 2, TOK, HEAD), BF16),
            pltpu.VMEM((Q_HEADS * TOK, HEAD), F32),
            pltpu.VMEM((Q_HEADS * TOK, 128), F32),
            pltpu.VMEM((Q_HEADS * TOK, 128), F32),
            sem((4,)),
            sem((3, NFT)),
            sem((3, 2)),
            sem((4, 2)),
            sem((2, 2, NRS)),
            sem((2, 2, NRS)),
            sem((2, 2, NAG)),
            sem((2, 2, NAG)),
        ],
        compiler_params=pltpu.CompilerParams(
            collective_id=layer, has_side_effects=True, vmem_limit_bytes=67043328),
    )(x, rope, *weights, norm_gain, qk_gain)


def solution(mesh):
    row_spec = P(('dp', 'cp'), None)
    col_spec = P(None, None, 'tp')
    row_w_spec = P(None, 'tp', None)
    cache_spec = P(None, ('dp', 'cp'), 'tp', None)

    def device_fn(hidden, positions, w_q, w_k, w_v, w_o, w_gate, w_up, w_down, norm_gain, qk_gain):
        pos = positions.astype(F32)[:, None]
        exponent = -(jnp.arange(HALF, dtype=F32) * 2.0) / HEAD
        angles = jnp.stack([pos * (theta ** exponent) for theta in THETAS])
        rope = jnp.stack([jnp.cos(angles), jnp.sin(angles)], axis=1)
        weights = (w_q, w_k, w_v, w_o, w_gate, w_up, w_down)
        x1, k0, v0 = run_layer(0, hidden, rope, weights, norm_gain, qk_gain)
        x2, k1, v1 = run_layer(1, x1, rope, weights, norm_gain, qk_gain)
        return x2, jnp.stack([k0, k1])[:, :, None, :], jnp.stack([v0, v1])[:, :, None, :]

    return jax.shard_map(
        device_fn,
        mesh=mesh,
        in_specs=(row_spec, P(('dp', 'cp')), col_spec, col_spec, col_spec, row_w_spec, col_spec, col_spec, row_w_spec, P(), P()),
        out_specs=(row_spec, cache_spec, cache_spec),
        check_vma=False,
    )
```

```python
import functools
import jax
import jax.numpy as jnp
import numpy as np
from jax import lax
from jax.experimental import pallas as pl
from jax.experimental.pallas import tpu as pltpu
from jax.sharding import PartitionSpec as P

MESH = pl.DeviceIdType.MESH
THETAS = (10000.0, 1000000.0)
EPS = 1e-6
NEG_BIG = -1e30
TOK = 256
D = 2304
HEAD = 256
HALF = 128
Q_HEADS = 2
FT = 256
NFT = D // FT
RS = 8
NRS = 128 // RS
AG = 16
NAG = 128 // AG
RS_LAG = 4
AG_LAG = 4
F32 = jnp.float32
BF16 = jnp.bfloat16


def norm_rows(src, gain, dst, rows=16):
    def body(i, carry):
        sl = pl.ds(pl.multiple_of(i * rows, rows), rows)
        vals = src[sl, :].astype(F32)
        mean_sq = jnp.mean(vals * vals, axis=-1, keepdims=True)
        dst[sl, :] = (vals * lax.rsqrt(mean_sq + EPS) * gain).astype(BF16)
        return carry

    lax.fori_loop(0, TOK // rows, body, 0)


def head_norm_rope(vals, gain, cosine, sine):
    mean_sq = jnp.mean(vals * vals, axis=-1, keepdims=True)
    vals = vals * lax.rsqrt(mean_sq + EPS) * gain
    low, high = vals[:, :HALF], vals[:, HALF:]
    return jnp.concatenate([low * cosine - high * sine, high * cosine + low * sine], axis=-1).astype(BF16)


def reduce_norm_share(z, part, land, res, gain, out, sems):
    rs_send, rs_recv, ag_send, ag_recv = sems

    def towards(flow):
        return z + 1 if flow else z - 1

    def away(flow):
        return z - 1 if flow else z + 1

    def rs_copy(flow, c):
        rows = pl.ds(pl.multiple_of(128 * flow + c * RS, RS), RS)
        return pltpu.make_async_remote_copy(
            src_ref=part.at[rows], dst_ref=land.at[rows], send_sem=rs_send.at[flow, c],
            recv_sem=rs_recv.at[flow, c], device_id={'tp': towards(flow)}, device_id_type=MESH)

    def ag_copy(flow, c):
        rows = pl.ds(pl.multiple_of(128 * flow + c * AG, AG), AG)
        return pltpu.make_async_remote_copy(
            src_ref=out.at[rows], dst_ref=out.at[rows], send_sem=ag_send.at[flow, c],
            recv_sem=ag_recv.at[flow, c], device_id={'tp': away(flow)}, device_id_type=MESH)

    def take(flow, c):
        rs_copy(flow, c).wait_recv()
        rows = pl.ds(pl.multiple_of(128 * flow + c * RS, RS), RS)
        part[rows, :] = part[rows, :] + land[rows, :]

    def hop(flow, c):
        take(flow, c)
        rs_copy(flow, c).start()

    def relay(flow, c):
        ag_copy(flow, c).wait_recv()
        ag_copy(flow, c).start()

    def loop(n, fn, start=0):
        def body(i, carry):
            fn(i)
            return carry
        lax.fori_loop(start, n, body, 0)

    def end_role(source, final):
        loop(NRS, lambda c: rs_copy(source, c).start())

        def finish(c):
            for i in range(AG // RS):
                take(final, c * (AG // RS) + i)
            rows = pl.ds(pl.multiple_of(128 * final + c * AG, AG), AG)
            vals = part[rows, :]
            mean_sq = jnp.mean(vals * vals, axis=-1, keepdims=True)
            out[rows, :] = (res[rows, :].astype(F32) + vals * lax.rsqrt(mean_sq + EPS) * gain).astype(BF16)
            ag_copy(final, c).start()

        loop(NAG, finish)
        loop(NAG, lambda c: ag_copy(source, c).wait_recv())
        loop(NRS, lambda c: rs_copy(source, c).wait_send())
        loop(NAG, lambda c: ag_copy(final, c).wait_send())

    def mid_role(near, far):
        def lagged(n, lag, first, second):
            loop(lag, first)

            def both(c):
                first(c)
                second(c - lag)

            loop(n, both, lag)
            loop(n, second, n - lag)

        lagged(NRS, RS_LAG, lambda c: hop(near, c), lambda c: hop(far, c))
        lagged(NAG, AG_LAG, lambda c: relay(far, c), lambda c: relay(near, c))
        loop(NRS, lambda c: rs_copy(near, c).wait_send())
        loop(NRS, lambda c: rs_copy(far, c).wait_send())
        loop(NAG, lambda c: ag_copy(near, c).wait_send())
        loop(NAG, lambda c: ag_copy(far, c).wait_send())

    pl.when(z == 0)(lambda: end_role(1, 0))
    pl.when(z == 1)(lambda: mid_role(1, 0))
    pl.when(z == 2)(lambda: mid_role(0, 1))
    pl.when(z == 3)(lambda: end_role(0, 1))


def layer_kernel(layer, x_ref, cos_ref, sin_ref, wq_hbm, wk_hbm, wv_hbm, wo_hbm, wg_hbm, wu_hbm, wd_hbm, gain_ref, qk_ref,
                 x_out, k_out, v_out,
                 wq, wk, wv, wo, wg, wu, wd, h_buf, r_buf, s_buf, part, land, q_buf, kv, acc, run_max, run_sum,
                 w_sem, t_sem, kv_send, kv_recv, rs_send, rs_recv, ag_send, ag_recv):
    z = lax.axis_index('tp')
    me = lax.axis_index('cp')
    twin = me + 1 - 2 * lax.rem(me, 2)
    across = lax.rem(me + 2, 4)

    barrier = pltpu.get_barrier_semaphore()
    pl.when(z > 0)(lambda: pl.semaphore_signal(barrier, inc=1, device_id={'tp': z - 1}, device_id_type=MESH))
    pl.when(z < 3)(lambda: pl.semaphore_signal(barrier, inc=1, device_id={'tp': z + 1}, device_id_type=MESH))
    pl.semaphore_signal(barrier, inc=1, device_id={'cp': twin}, device_id_type=MESH)
    pl.semaphore_signal(barrier, inc=1, device_id={'cp': across}, device_id_type=MESH)

    loads = [pltpu.make_async_copy(src.at[layer], dst, w_sem.at[i])
             for i, (src, dst) in enumerate(((wk_hbm, wk), (wv_hbm, wv), (wq_hbm, wq), (wo_hbm, wo)))]
    for copy in loads:
        copy.start()

    def tile_load(kind, src, dst, t):
        cols = pl.ds(pl.multiple_of(t * FT, FT), FT)
        return pltpu.make_async_copy(src.at[layer, :, cols], dst.at[t], t_sem.at[kind, t])

    def start_gate_up(t, carry):
        tile_load(0, wg_hbm, wg, t).start()
        tile_load(1, wu_hbm, wu, t).start()
        return carry

    def start_down(t, carry):
        tile_load(2, wd_hbm, wd, t).start()
        return carry

    lax.fori_loop(0, NFT, start_gate_up, 0)
    lax.fori_loop(0, NFT, start_down, 0)

    gains = [1.0 + gain_ref[layer, i:i + 1, :] for i in range(4)]
    q_gain = 1.0 + qk_ref[layer, 0:1, :]
    k_gain = 1.0 + qk_ref[layer, 1:2, :]
    cosine, sine = cos_ref[layer], sin_ref[layer]

    norm_rows(x_ref, gains[0], h_buf)
    state = h_buf[...]

    loads[0].wait()
    k_rot = head_norm_rope(jnp.dot(state, wk[...], preferred_element_type=F32), k_gain, cosine, sine)
    kv[me, 0] = k_rot
    k_out[...] = k_rot
    loads[1].wait()
    v_rows = jnp.dot(state, wv[...], preferred_element_type=F32).astype(BF16)
    kv[me, 1] = v_rows
    v_out[...] = v_rows

    near_count = jnp.where(z > 0, 1, 0) + jnp.where(z < 3, 1, 0)
    pl.semaphore_wait(barrier, near_count + 2)

    def kv_copy(slot, part_id, lane, target):
        return pltpu.make_async_remote_copy(
            src_ref=kv.at[slot, part_id], dst_ref=kv.at[slot, part_id], send_sem=kv_send.at[lane, part_id],
            recv_sem=kv_recv.at[slot, part_id], device_id={'cp': target}, device_id_type=MESH)

    def send_own():
        for i in range(2):
            pl.when(me < 2)(lambda: kv_copy(me, i, 1, across).start())
            pl.when(lax.rem(me, 2) == 0)(lambda: kv_copy(me, i, 0, twin).start())

    send_own()

    loads[2].wait()
    q_all = jnp.dot(state, wq[...], preferred_element_type=F32)
    for i in range(Q_HEADS):
        q_buf[i * TOK:(i + 1) * TOK, :] = head_norm_rope(
            q_all[:, i * HEAD:(i + 1) * HEAD], q_gain, cosine, sine)

    def scores_of(slot):
        return lax.dot_general(q_buf[...], kv[slot, 0], (((1,), (1,)), ((), ())),
                               preferred_element_type=F32) * (HEAD ** -0.5)

    def first_block():
        scores = scores_of(me)
        row = lax.broadcasted_iota(jnp.int32, (Q_HEADS, TOK, TOK), 1).reshape(Q_HEADS * TOK, TOK)
        col = lax.broadcasted_iota(jnp.int32, (Q_HEADS * TOK, TOK), 1)
        scores = jnp.where(row >= col, scores, NEG_BIG)
        top = jnp.max(scores, axis=-1, keepdims=True)
        prob = jnp.exp(scores - top)
        run_max[...] = jnp.broadcast_to(top, run_max.shape)
        run_sum[...] = jnp.broadcast_to(jnp.sum(prob, axis=-1, keepdims=True), run_sum.shape)
        acc[...] = jnp.dot(prob.astype(BF16), kv[me, 1], preferred_element_type=F32)

    def next_block(slot):
        scores = scores_of(slot)
        old = run_max[:, :1]
        top = jnp.maximum(old, jnp.max(scores, axis=-1, keepdims=True))
        prob = jnp.exp(scores - top)
        factor = jnp.exp(old - top)
        run_max[...] = jnp.broadcast_to(top, run_max.shape)
        run_sum[...] = run_sum[...] * factor + jnp.sum(prob, axis=-1, keepdims=True)
        acc[...] = acc[...] * factor + jnp.dot(prob.astype(BF16), kv[slot, 1], preferred_element_type=F32)

    first_block()

    def recv(slot):
        for i in range(2):
            kv_copy(slot, i, 0, twin).wait_recv()

    def relay(slot):
        for i in range(2):
            kv_copy(slot, i, 0, twin).wait_recv()
            kv_copy(slot, i, 2, twin).start()

    def sent(lane, slot):
        for i in range(2):
            kv_copy(slot, i, lane, twin).wait_send()

    @pl.when(me == 0)
    def _():
        sent(0, 0)
        sent(1, 0)

    @pl.when(me == 1)
    def _():
        recv(0)
        next_block(0)
        sent(1, 1)

    @pl.when(me == 2)
    def _():
        relay(0)
        next_block(0)
        recv(1)
        next_block(1)
        sent(0, 2)
        sent(2, 0)

    @pl.when(me == 3)
    def _():
        recv(2)
        next_block(2)
        relay(1)
        next_block(1)
        recv(0)
        next_block(0)
        sent(2, 1)

    loads[3].wait()
    for i in range(Q_HEADS):
        rows = slice(i * TOK, (i + 1) * TOK)
        s_buf[:, i * HEAD:(i + 1) * HEAD] = (acc[rows, :] / run_sum[rows, :1]).astype(BF16)
    part[...] = jnp.dot(s_buf[:, :Q_HEADS * HEAD], wo[...], preferred_element_type=F32)

    def phase(n):
        return (rs_send.at[n], rs_recv.at[n], ag_send.at[n], ag_recv.at[n])

    reduce_norm_share(z, part, land, x_ref, gains[1], r_buf, phase(0))

    norm_rows(r_buf, gains[2], h_buf)

    def gate_up(t, carry):
        tile_load(0, wg_hbm, wg, t).wait()
        tile_load(1, wu_hbm, wu, t).wait()
        gate = jnp.dot(h_buf[...], wg[t], preferred_element_type=F32)
        up = jnp.dot(h_buf[...], wu[t], preferred_element_type=F32)
        s_buf[:, pl.ds(pl.multiple_of(t * FT, FT), FT)] = (jax.nn.gelu(gate, approximate=True) * up).astype(BF16)
        return carry

    lax.fori_loop(0, NFT, gate_up, 0)

    def down(t, carry):
        tile_load(2, wd_hbm, wd, t).wait()
        part[:, pl.ds(pl.multiple_of(t * FT, FT), FT)] = jnp.dot(s_buf[...], wd[t], preferred_element_type=F32)
        return carry

    lax.fori_loop(0, NFT, down, 0)

    reduce_norm_share(z, part, land, r_buf, gains[3], x_out, phase(1))


def run_layer(layer, x, rope, weights, norm_gain, qk_gain):
    vmem = pl.BlockSpec(memory_space=pltpu.VMEM)
    hbm = pl.BlockSpec(memory_space=pl.ANY)
    sem = pltpu.SemaphoreType.DMA
    return pl.pallas_call(
        functools.partial(layer_kernel, layer),
        name=f'layer_{layer}',
        out_shape=(
            jax.ShapeDtypeStruct((TOK, D), BF16),
            jax.ShapeDtypeStruct((TOK, HEAD), BF16),
            jax.ShapeDtypeStruct((TOK, HEAD), BF16),
        ),
        in_specs=[vmem] * 3 + [hbm] * 7 + [vmem, vmem],
        out_specs=(vmem, vmem, vmem),
        scratch_shapes=[
            pltpu.VMEM((D, Q_HEADS * HEAD), BF16),
            pltpu.VMEM((D, HEAD), BF16),
            pltpu.VMEM((D, HEAD), BF16),
            pltpu.VMEM((Q_HEADS * HEAD, D), BF16),
            pltpu.VMEM((NFT, D, FT), BF16),
            pltpu.VMEM((NFT, D, FT), BF16),
            pltpu.VMEM((NFT, D, FT), BF16),
            pltpu.VMEM((TOK, D), BF16),
            pltpu.VMEM((TOK, D), BF16),
            pltpu.VMEM((TOK, D), BF16),
            pltpu.VMEM((TOK, D), F32),
            pltpu.VMEM((TOK, D), F32),
            pltpu.VMEM((Q_HEADS * TOK, HEAD), BF16),
            pltpu.VMEM((4, 2, TOK, HEAD), BF16),
            pltpu.VMEM((Q_HEADS * TOK, HEAD), F32),
            pltpu.VMEM((Q_HEADS * TOK, 128), F32),
            pltpu.VMEM((Q_HEADS * TOK, 128), F32),
            sem((4,)),
            sem((3, NFT)),
            sem((3, 2)),
            sem((4, 2)),
            sem((2, 2, NRS)),
            sem((2, 2, NRS)),
            sem((2, 2, NAG)),
            sem((2, 2, NAG)),
        ],
        compiler_params=pltpu.CompilerParams(
            collective_id=layer, has_side_effects=True, vmem_limit_bytes=67043328),
    )(x, *rope, *weights, norm_gain, qk_gain)


def pack_kernel(x_in, k0, k1, v0, v1, x_out, k_out, v_out, sem):
    copies = [pltpu.make_async_copy(src, dst, sem.at[i]) for i, (src, dst) in enumerate((
        (x_in, x_out), (k0, k_out.at[0]), (k1, k_out.at[1]), (v0, v_out.at[0]), (v1, v_out.at[1])))]
    for copy in copies:
        copy.start()
    for copy in copies:
        copy.wait()


def pack(*arrays):
    cache = jax.ShapeDtypeStruct((2, TOK, HEAD), BF16)
    return pl.pallas_call(
        pack_kernel,
        name='pack',
        out_shape=(jax.ShapeDtypeStruct((TOK, D), BF16), cache, cache),
        in_specs=[pl.BlockSpec(memory_space=pltpu.VMEM)] * 5,
        out_specs=(pl.BlockSpec(memory_space=pl.ANY),) * 3,
        scratch_shapes=[pltpu.SemaphoreType.DMA((5,))],
    )(*arrays)


def solution(mesh):
    row_spec = P(('dp', 'cp'), None)
    col_spec = P(None, None, 'tp')
    row_w_spec = P(None, 'tp', None)
    cache_spec = P(None, ('dp', 'cp'), 'tp', None)

    def device_fn(hidden, positions, w_q, w_k, w_v, w_o, w_gate, w_up, w_down, norm_gain, qk_gain):
        pos = (positions[0] + lax.broadcasted_iota(jnp.int32, (TOK, HALF), 0)).astype(F32)
        exponent = -(np.arange(HALF) * 2.0) / HEAD
        inv_freq = np.stack([theta ** exponent for theta in THETAS]).astype(np.float32)
        angles = pos * inv_freq[:, None, :]
        rope = (jnp.cos(angles), jnp.sin(angles))
        weights = (w_q, w_k, w_v, w_o, w_gate, w_up, w_down)
        x1, k0, v0 = run_layer(0, hidden, rope, weights, norm_gain, qk_gain)
        x2, k1, v1 = run_layer(1, x1, rope, weights, norm_gain, qk_gain)
        x2, k_cache, v_cache = pack(x2, k0, k1, v0, v1)
        return x2, k_cache[:, :, None, :], v_cache[:, :, None, :]

    return jax.shard_map(
        device_fn,
        mesh=mesh,
        in_specs=(row_spec, P(('dp', 'cp')), col_spec, col_spec, col_spec, row_w_spec, col_spec, col_spec, row_w_spec, P(), P()),
        out_specs=(row_spec, cache_spec, cache_spec),
        check_vma=False,
    )
```
